32 devices in a mesh: grp: 8 (over z, x), tbl: 4 (over y, core).
Axes of the slice: x: 2, y: 2, z: 4, core: 2. Of those that a mesh axis runs over, the one named last changes fastest.
Arguments:
- next_ids: int32 [4096, 224], P(('grp', 'tbl')), may hold values from 0 to 6143
- next_lengths: int32 [4096, 26], P(('grp', 'tbl')), may hold values from 1 to 8
- slot_of_table: int32 [26], replicated, may hold values from 0 to 27, as said below
- tables: bfloat16 [28, 6144, 128], P('tbl'), may hold values from -2.5 to 2.5
- cross_input: bfloat16 [4096, 3456], P(('grp', 'tbl')), may hold values from -6 to 6
- cotangent: bfloat16 [4096, 3456], P(('grp', 'tbl')), may hold values from -6 to 6
- up_weight: bfloat16 [256, 3456], replicated, may hold values from -0.375 to 0.375
- down_weight: bfloat16 [3456, 256], replicated, may hold values from -0.109375 to 0.109375
Outputs:
- next_embedded: bfloat16 [4096, 3328], P(('grp', 'tbl'))
- grad_up: float32 [256, 3456], P('tbl', 'grp')
- grad_down: float32 [3456, 256], P('grp', 'tbl')
The draws below stay inside these ranges and needn't reach their ends.
Inputs may be any that keep to these rules, and one draw needn't show every extreme that they name: `next_ids`: entry 8 * s + k of an example's row is the k-th id of the bag held in slot s; entries with k at or past the bag's length, and all entries of slots that hold no table, are padding. `slot_of_table`: distinct slots; owner o along tbl holds slots o * 7 to o * 7 + 6, so an owner holds up to 7 tables and some owner holds exactly 7.
All inputs are finite; a program needn't handle non-finite values.
Results may differ from the reference program's by a relative error of at most 0.0049.
Values may be sent and summed in bfloat16 or wider, within the bound.
A program may use at most 128 MiB of HBM per device.

```python
import math
import jax
import jax.numpy as jnp
import numpy as np
from jax import lax

F = 26
E = 128
R = 256
MAXLEN = 8
ROWS = 6144
B_DEV = 128
D = 3456
TOKENS = 4096
SLOTS_ALL = 28
N_TBL = 4


def draw_slot_of_table(key, part):
    return jax.random.permutation(key, SLOTS_ALL)[:F].astype(jnp.int32)


def plant(entries, stream_key, smallest, top_value):
    shape = entries.shape
    place = [jax.random.randint(jax.random.fold_in(stream_key, axis), (), 0, shape[axis]) for axis in range(len(shape))]
    entries = entries.at[tuple(place)].set(smallest)
    longest = shape.index(max(shape))
    place[longest] = (place[longest] + 1) % shape[longest]
    return entries.at[tuple(place)].set(top_value)


def block_scale(stream_key, shape, split, low, largest):
    loudness, own = 1.0, jax.random.fold_in(stream_key, 6)
    for dim, shards_of in split:
        heights = jnp.exp(jax.random.uniform(jax.random.fold_in(own, dim), (shards_of,), jnp.float32, low / len(split), largest / len(split)))
        loudness = loudness * jnp.repeat(heights, shape[dim] // shards_of).reshape([-1 if axis == dim else 1 for axis in range(len(shape))])
    return loudness


def cumulative_ranks(amount, slope):
    loads = [(1 << 20) // math.isqrt(standing ** slope) + 1 for standing in range(1, amount + 1)]
    deviation = 1 + sum(loads) // (1 << 30)
    return np.cumsum(np.array([max(1, weight // deviation) for weight in loads]))


def ranked_ids(key, extent, number_of, lean):
    table = cumulative_ranks(number_of, lean)
    pick = jax.random.randint(jax.random.fold_in(key, 1), extent, 0, int(table[number_of - 1]))
    grade = jnp.searchsorted(jnp.asarray(table, jnp.int32), pick, side="right")
    return jax.random.permutation(jax.random.fold_in(key, 2), number_of)[grade].astype(jnp.int32)


def gaussian(rng, extent, width, most, cuts=(), kind=jnp.bfloat16):
    entries = jax.random.normal(rng, extent, jnp.float32) * width
    if len(cuts) > 0:
        entries = block_scale(rng, extent, cuts, -0.22, 0.18) * entries
    return jnp.clip(entries, min=-most, max=most).astype(kind)


def setup_inputs(seed: int = 0) -> dict:
    key_list = jax.random.split(jax.random.key(seed), 9)
    return {
        "next_ids": plant(ranked_ids(key_list[0], (TOKENS, SLOTS_ALL * MAXLEN), ROWS, 2), jax.random.fold_in(key_list[0], 3), 0, ROWS - 1).astype(jnp.int32),
        "next_lengths": plant(jax.random.randint(key_list[1], (TOKENS, F), 1, MAXLEN + 1), jax.random.fold_in(key_list[1], 1), 1, MAXLEN).astype(jnp.int32),
        "slot_of_table": draw_slot_of_table(jax.random.fold_in(key_list[8], 71), 0),
        "tables": gaussian(key_list[3], (SLOTS_ALL, ROWS, E), 0.35, 2.5, ((0, 4),)),
        "cross_input": gaussian(key_list[4], (TOKENS, D), 1.0, 6.0, ((0, 32),)),
        "cotangent": gaussian(key_list[5], (TOKENS, D), 1.0, 6.0, ((0, 32),)),
        "up_weight": gaussian(key_list[6], (R, D), R ** -0.5, 0.375),
        "down_weight": gaussian(key_list[7], (D, R), D ** -0.5, 0.109375),
    }


def pool_block(tables, slot_of_table, ids, lengths):
    count = ids.shape[0]
    ids_three = ids.reshape(count, SLOTS_ALL, MAXLEN)
    chosen = jnp.take(ids_three, slot_of_table, axis=1)
    flat_table = tables.reshape(SLOTS_ALL * ROWS, E)
    index = (chosen + (slot_of_table * ROWS)[None, :, None]).astype(jnp.int32)
    picked = jnp.take(flat_table, index.reshape(-1), axis=0).reshape(count, F, MAXLEN, E)
    keep = lax.broadcasted_iota(jnp.int32, (count, F, MAXLEN), 2) < lengths[:, :, None]
    masked = jnp.where(keep[..., None], picked, jnp.zeros((), picked.dtype))
    pooled = lax.optimization_barrier(jnp.sum(masked.astype(jnp.float32), axis=2))
    return pooled.astype(jnp.bfloat16).reshape(count, F * E)

def reference(next_ids, next_lengths, slot_of_table, tables, cross_input, cotangent, up_weight, down_weight):
    blocks = TOKENS // B_DEV
    id_blocks = next_ids.reshape(blocks, B_DEV, SLOTS_ALL * MAXLEN)
    len_blocks = next_lengths.reshape(blocks, B_DEV, F)
    pooled = lax.map(lambda pair: pool_block(tables, slot_of_table, pair[0], pair[1]), (id_blocks, len_blocks))
    next_embedded = pooled.reshape(TOKENS, F * E)
    span = B_DEV * N_TBL
    input_blocks = cross_input.reshape(TOKENS // span, span, D)
    grad_blocks = cotangent.reshape(TOKENS // span, span, D)

    def step(carry, pair):
        total_up, total_down = carry
        inputs, grads = pair
        low = jnp.dot(inputs, down_weight, preferred_element_type=jnp.float32).astype(jnp.bfloat16)
        dz = (grads.astype(jnp.float32) * inputs.astype(jnp.float32)).astype(jnp.bfloat16)
        dlow = jnp.dot(dz, up_weight.T, preferred_element_type=jnp.float32).astype(jnp.bfloat16)
        total_up = total_up + jnp.dot(low.T, dz, preferred_element_type=jnp.float32)
        total_down = total_down + jnp.dot(inputs.T, dlow, preferred_element_type=jnp.float32)
        return ((total_up, total_down), None)
    start = (jnp.zeros((R, D), jnp.float32), jnp.zeros((D, R), jnp.float32))
    (total_up, total_down), unused = lax.scan(step, start, (input_blocks, grad_blocks))
    factor = 1.0 / math.sqrt(TOKENS)
    return (next_embedded, total_up * factor, total_down * factor)
```

```python
import functools
import math

import jax
import jax.numpy as jnp
from jax import lax
from jax.experimental import pallas as pl
from jax.experimental.pallas import tpu as pltpu
from jax.sharding import PartitionSpec as P

LANES = 128


def pool_kernel(maxlen, idx_ref, tab_ref, out_ref, stage, wide, acc, sem):
    owners, batch, _ = out_ref.shape
    slots, rows, width = tab_ref.shape
    per_line = LANES // maxlen
    lines = batch // per_line
    chunk = 256

    def fetch(s):
        return pltpu.make_async_copy(tab_ref.at[s], stage.at[s % 2], sem.at[s % 2])

    fetch(0).start()
    wide[pl.ds(rows, 8), :] = jnp.zeros((8, width), jnp.float32)
    for s in range(slots):
        if s + 1 < slots:
            fetch(s + 1).start()
        fetch(s).wait()

        @pl.loop(0, rows // chunk)
        def _(c):
            at = pl.ds(pl.multiple_of(c * chunk, chunk), chunk)
            wide[at, :] = stage[s % 2, at, :].astype(jnp.float32)

        @pl.loop(0, owners * lines)
        def _(g):
            src = g // lines
            line = s * lines + g % lines
            for u in range(per_line):
                got = [
                    wide[pl.ds(idx_ref[src, line, u * maxlen + k], 1), :] for k in range(maxlen)
                ]
                while len(got) > 1:
                    got = [a + b for a, b in zip(got[::2], got[1::2])] + (
                        [got[-1]] if len(got) % 2 else []
                    )
                acc[pl.ds(g * per_line + u, 1), :] = got[0]

        for o in range(owners):
            out_ref[o, :, s * width : (s + 1) * width] = acc[
                o * batch : (o + 1) * batch, :
            ].astype(jnp.bfloat16)


def pool(idx, tables, batch, maxlen):
    slots, rows, width = tables.shape
    owners = idx.shape[0]
    return pl.pallas_call(
        functools.partial(pool_kernel, maxlen),
        out_shape=jax.ShapeDtypeStruct((owners, batch, slots * width), jnp.bfloat16),
        in_specs=[
            pl.BlockSpec(memory_space=pltpu.SMEM),
            pl.BlockSpec(memory_space=pl.ANY),
        ],
        out_specs=pl.BlockSpec(memory_space=pltpu.VMEM),
        scratch_shapes=[
            pltpu.VMEM((2, rows, width), jnp.bfloat16),
            pltpu.VMEM((rows + 8, width), jnp.float32),
            pltpu.VMEM((owners * batch, width), jnp.float32),
            pltpu.SemaphoreType.DMA((2,)),
        ],
        compiler_params=pltpu.CompilerParams(vmem_limit_bytes=60 << 20),
        cost_estimate=pl.CostEstimate(
            flops=100_000_000, bytes_accessed=tables.size * 2, transcendentals=0
        ),
        name="pool",
    )(idx, tables)


def order_kernel(slot_ref, got_ref, out_ref):
    owners, batch, wide = got_ref.shape
    feats = slot_ref.shape[0]
    width = out_ref.shape[1] // feats
    slots = wide // width
    for f in range(feats):
        s = slot_ref[f]
        at = pl.ds(pl.multiple_of(lax.rem(s, slots) * width, width), width)
        out_ref[:, f * width : (f + 1) * width] = got_ref[lax.div(s, slots), :, at]


def order(slot_of_table, got, width):
    return pl.pallas_call(
        order_kernel,
        out_shape=jax.ShapeDtypeStruct(
            (got.shape[1], slot_of_table.shape[0] * width), jnp.bfloat16
        ),
        in_specs=[
            pl.BlockSpec(memory_space=pltpu.SMEM),
            pl.BlockSpec(memory_space=pltpu.VMEM),
        ],
        out_specs=pl.BlockSpec(memory_space=pltpu.VMEM),
        name="order",
    )(slot_of_table, got)


def bag_rows(next_ids, next_lengths, slot_of_table, slots, owners, rows):
    batch = next_ids.shape[0]
    slots_all = slots * owners
    maxlen = next_ids.shape[1] // slots_all
    hit = (slot_of_table[:, None] == lax.broadcasted_iota(jnp.int32, (1, slots_all), 1)).astype(
        jnp.int32
    )
    slot_lengths = jnp.sum(next_lengths[:, :, None] * hit[None, :, :], axis=1)
    keep = lax.broadcasted_iota(jnp.int32, (batch, slots_all, maxlen), 2) < slot_lengths[:, :, None]
    idx = jnp.where(keep, next_ids.reshape(batch, slots_all, maxlen), rows)
    return idx.transpose(1, 0, 2).reshape(owners, slots * batch * maxlen // LANES, LANES)


def on_device(
    next_ids, next_lengths, slot_of_table, tables, cross_input, cotangent, up_weight, down_weight
):
    batch = next_ids.shape[0]
    owners = lax.axis_size("tbl")
    slots, rows, width = tables.shape
    maxlen = next_ids.shape[1] // (slots * owners)
    idx = bag_rows(next_ids, next_lengths, slot_of_table, slots, owners, rows)
    low = jnp.dot(cross_input, down_weight, preferred_element_type=jnp.float32).astype(jnp.bfloat16)
    dz = (cotangent.astype(jnp.float32) * cross_input.astype(jnp.float32)).astype(jnp.bfloat16)
    dlow = jnp.dot(dz, up_weight.T, preferred_element_type=jnp.float32).astype(jnp.bfloat16)
    total = batch * lax.axis_size("grp") * owners
    factor = 1.0 / math.sqrt(total)
    part_up = jnp.dot(low.T, dz, preferred_element_type=jnp.float32) * factor
    part_down = jnp.dot(cross_input.T, dlow, preferred_element_type=jnp.float32) * factor
    part_up, part_down = part_up.astype(jnp.bfloat16), part_down.astype(jnp.bfloat16)
    owner_up, owner_down = (
        lax.psum_scatter(part_up, "tbl", scatter_dimension=0, tiled=True).astype(jnp.float32),
        lax.psum_scatter(part_down, "tbl", scatter_dimension=1, tiled=True).astype(jnp.float32),
    )
    got_idx = lax.all_to_all(idx, "tbl", split_axis=0, concat_axis=0, tiled=True)
    pooled = pool(got_idx, tables, batch, maxlen)
    returned = lax.all_to_all(pooled, "tbl", split_axis=0, concat_axis=0, tiled=True)
    next_embedded = order(slot_of_table, returned, width)
    grad_up, grad_down = (
        lax.psum_scatter(owner_up, "grp", scatter_dimension=1, tiled=True),
        lax.psum_scatter(owner_down, "grp", scatter_dimension=0, tiled=True),
    )
    return (next_embedded, grad_up, grad_down)


def solution(mesh):
    return jax.shard_map(
        on_device,
        mesh=mesh,
        in_specs=(
            P(("grp", "tbl"), None),
            P(("grp", "tbl"), None),
            P(),
            P("tbl", None, None),
            P(("grp", "tbl"), None),
            P(("grp", "tbl"), None),
            P(),
            P(),
        ),
        out_specs=(P(("grp", "tbl"), None), P("tbl", "grp"), P("grp", "tbl")),
        check_vma=False,
    )
```

```python
import functools
import math

import jax
import jax.numpy as jnp
from jax import lax
from jax.experimental import pallas as pl
from jax.experimental.pallas import tpu as pltpu
from jax.sharding import PartitionSpec as P

LANES = 128


def pool_kernel(maxlen, idx_ref, tab_ref, out_ref, stage, wide, acc, sem):
    owners, batch, _ = out_ref.shape
    slots, rows, width = tab_ref.shape
    per_line = LANES // maxlen
    lines = batch // per_line
    chunk = 256

    def fetch(s):
        return pltpu.make_async_copy(tab_ref.at[s], stage.at[s % 2], sem.at[s % 2])

    fetch(0).start()
    wide[pl.ds(rows, 8), :] = jnp.zeros((8, width), jnp.float32)
    for s in range(slots):
        if s + 1 < slots:
            fetch(s + 1).start()
        fetch(s).wait()

        @pl.loop(0, rows // chunk)
        def _(c):
            at = pl.ds(pl.multiple_of(c * chunk, chunk), chunk)
            wide[at, :] = stage[s % 2, at, :].astype(jnp.float32)

        @pl.loop(0, owners * lines)
        def _(g):
            src = g // lines
            line = s * lines + g % lines
            for u in range(per_line):
                got = [
                    wide[pl.ds(idx_ref[src, line, u * maxlen + k], 1), :] for k in range(maxlen)
                ]
                while len(got) > 1:
                    got = [a + b for a, b in zip(got[::2], got[1::2])] + (
                        [got[-1]] if len(got) % 2 else []
                    )
                acc[pl.ds(g * per_line + u, 1), :] = got[0]

        for o in range(owners):
            out_ref[o, :, s * width : (s + 1) * width] = acc[
                o * batch : (o + 1) * batch, :
            ].astype(jnp.bfloat16)


def pool(idx, tables, batch, maxlen):
    slots, rows, width = tables.shape
    owners = idx.shape[0]
    return pl.pallas_call(
        functools.partial(pool_kernel, maxlen),
        out_shape=jax.ShapeDtypeStruct((owners, batch, slots * width), jnp.bfloat16),
        in_specs=[
            pl.BlockSpec(memory_space=pltpu.SMEM),
            pl.BlockSpec(memory_space=pl.ANY),
        ],
        out_specs=pl.BlockSpec(memory_space=pltpu.VMEM),
        scratch_shapes=[
            pltpu.VMEM((2, rows, width), jnp.bfloat16),
            pltpu.VMEM((rows + 8, width), jnp.float32),
            pltpu.VMEM((owners * batch, width), jnp.float32),
            pltpu.SemaphoreType.DMA((2,)),
        ],
        compiler_params=pltpu.CompilerParams(vmem_limit_bytes=60 << 20),
        cost_estimate=pl.CostEstimate(
            flops=100_000_000, bytes_accessed=tables.size * 2, transcendentals=0
        ),
        name="pool",
    )(idx, tables)


def order_kernel(slot_ref, got_ref, out_ref):
    owners, batch, wide = got_ref.shape
    feats = slot_ref.shape[0]
    width = out_ref.shape[1] // feats
    slots = wide // width
    for f in range(feats):
        s = slot_ref[f]
        at = pl.ds(pl.multiple_of(lax.rem(s, slots) * width, width), width)
        out_ref[:, f * width : (f + 1) * width] = got_ref[lax.div(s, slots), :, at]


def order(slot_of_table, got, width):
    return pl.pallas_call(
        order_kernel,
        out_shape=jax.ShapeDtypeStruct(
            (got.shape[1], slot_of_table.shape[0] * width), jnp.bfloat16
        ),
        in_specs=[
            pl.BlockSpec(memory_space=pltpu.SMEM),
            pl.BlockSpec(memory_space=pltpu.VMEM),
        ],
        out_specs=pl.BlockSpec(memory_space=pltpu.VMEM),
        name="order",
    )(slot_of_table, got)


def bag_rows(next_ids, next_lengths, slot_of_table, slots, owners, rows):
    batch = next_ids.shape[0]
    slots_all = slots * owners
    maxlen = next_ids.shape[1] // slots_all
    hit = (slot_of_table[:, None] == lax.broadcasted_iota(jnp.int32, (1, slots_all), 1)).astype(
        jnp.int32
    )
    slot_lengths = jnp.sum(next_lengths[:, :, None] * hit[None, :, :], axis=1)
    keep = lax.broadcasted_iota(jnp.int32, (batch, slots_all, maxlen), 2) < slot_lengths[:, :, None]
    idx = jnp.where(keep, next_ids.reshape(batch, slots_all, maxlen), rows)
    return idx.transpose(1, 0, 2).reshape(owners, slots * batch * maxlen // LANES, LANES)


def plain(
    next_ids, next_lengths, slot_of_table, tables, cross_input, cotangent, up_weight, down_weight
):
    batch = next_ids.shape[0]
    owners = lax.axis_size("tbl")
    slots, rows, width = tables.shape
    maxlen = next_ids.shape[1] // (slots * owners)
    idx = bag_rows(next_ids, next_lengths, slot_of_table, slots, owners, rows)
    low = jnp.dot(cross_input, down_weight, preferred_element_type=jnp.float32).astype(jnp.bfloat16)
    dz = (cotangent.astype(jnp.float32) * cross_input.astype(jnp.float32)).astype(jnp.bfloat16)
    dlow = jnp.dot(dz, up_weight.T, preferred_element_type=jnp.float32).astype(jnp.bfloat16)
    total = batch * lax.axis_size("grp") * owners
    factor = 1.0 / math.sqrt(total)
    part_up = jnp.dot(low.T, dz, preferred_element_type=jnp.float32) * factor
    part_down = jnp.dot(cross_input.T, dlow, preferred_element_type=jnp.float32) * factor
    part_up, part_down = part_up.astype(jnp.bfloat16), part_down.astype(jnp.bfloat16)
    owner_up, owner_down = (
        lax.psum_scatter(part_up, "tbl", scatter_dimension=0, tiled=True).astype(jnp.float32),
        lax.psum_scatter(part_down, "tbl", scatter_dimension=1, tiled=True).astype(jnp.float32),
    )
    got_idx = lax.all_to_all(idx, "tbl", split_axis=0, concat_axis=0, tiled=True)
    pooled = pool(got_idx, tables, batch, maxlen)
    returned = lax.all_to_all(pooled, "tbl", split_axis=0, concat_axis=0, tiled=True)
    next_embedded = order(slot_of_table, returned, width)
    grad_up, grad_down = (
        lax.psum_scatter(owner_up, "grp", scatter_dimension=1, tiled=True),
        lax.psum_scatter(owner_down, "grp", scatter_dimension=0, tiled=True),
    )
    return (next_embedded, grad_up, grad_down)


def step_kernel(
    maxlen,
    factor,
    split,
    checkpoints,
    idx_ref,
    slot_ref,
    tab_ref,
    x_ref,
    ct_ref,
    up_ref,
    down_ref,
    emb_ref,
    grad_ref,
    idx_in,
    idx_s,
    part,
    c_in,
    a_in,
    b_in,
    a2_in,
    b2_in,
    z_in,
    stage,
    wide,
    acc,
    pooled,
    got,
    tab_sem,
    smem_sem,
    idx_sem,
    core_sem,
    one_sem,
    two_sem,
    z_sem,
    pool_sem,
):
    owners, zs, _, high, lanes = part.shape
    slots, rows, width = tab_ref.shape
    batch = x_ref.shape[0]
    rank = down_ref.shape[1]
    cols = rank // owners
    per_line = LANES // maxlen
    lines = batch // per_line
    chunk = 256
    g, t = lax.axis_index("grp"), lax.axis_index("tbl")
    z, x = g // 2, g % 2
    core = t + 1 - 2 * (t % 2)
    far = (t + 2) % owners
    other = 1 - x
    side = g + 1 - 2 * x

    def fetch(s):
        return pltpu.make_async_copy(tab_ref.at[s], stage.at[s % 2], tab_sem.at[s % 2])

    def send(src, dst, sems, n, device):
        return pltpu.make_async_remote_copy(
            src_ref=src,
            dst_ref=dst,
            send_sem=sems.at[0, n],
            recv_sem=sems.at[1, n],
            device_id=device,
            device_id_type=pl.DeviceIdType.MESH,
        )

    fetch(0).start()
    barrier = pltpu.get_barrier_semaphore()
    near = [(g, (t + d) % owners) for d in range(1, owners)] + [(side, t)]
    near += [((z + d) % zs * 2 + x, t) for d in range(1, zs)]
    for device in near:
        pl.semaphore_signal(
            barrier, inc=1, device_id=device, device_id_type=pl.DeviceIdType.MESH
        )
    pl.semaphore_wait(barrier, len(near))

    ids_out = [
        send(idx_ref.at[(t + d) % owners], idx_in.at[t], idx_sem, d - 1, (g, (t + d) % owners))
        for d in range(1, owners)
    ]
    for copy in ids_out:
        copy.start()
    keep_ids = pltpu.make_async_copy(idx_ref.at[t], idx_s.at[t], smem_sem.at[0])
    keep_ids.start()

    low = jnp.dot(x_ref[...], down_ref[...], preferred_element_type=jnp.float32).astype(jnp.bfloat16)
    dz = (ct_ref[...].astype(jnp.float32) * x_ref[...].astype(jnp.float32)).astype(jnp.bfloat16)
    ct = dz
    dlow = lax.dot_general(
        dz, up_ref[...], (((1,), (1,)), ((), ())), preferred_element_type=jnp.float32
    ).astype(jnp.bfloat16)
    first = (((0,), (0,)), ((), ()))
    for block in range(2 * zs):
        begin = block * high
        edge = begin // LANES * LANES
        stop = -(-(begin + high) // LANES) * LANES
        up = lax.dot_general(ct[:, edge:stop], low, first, preferred_element_type=jnp.float32)
        down = lax.dot_general(
            x_ref[:, edge:stop], dlow, first, preferred_element_type=jnp.float32
        )
        up = (up[begin - edge : begin - edge + high] * factor).astype(jnp.bfloat16)
        down = (down[begin - edge : begin - edge + high] * factor).astype(jnp.bfloat16)
        for o in range(owners):
            part[o, block // 2, block % 2] = jnp.concatenate(
                [up[:, o * cols : (o + 1) * cols], down[:, o * cols : (o + 1) * cols]], axis=1
            )

    cross = [
        send(part.at[core], c_in.at[0], core_sem, 0, (g, core)),
        send(part.at[(core + 2) % owners], c_in.at[1], core_sem, 1, (g, core)),
    ]
    for copy in cross:
        copy.start()

    for copy in ids_out:
        copy.wait()
    keep_ids.wait()
    got_ids = [
        pltpu.make_async_copy(
            idx_in.at[(t + d) % owners], idx_s.at[(t + d) % owners], smem_sem.at[d]
        )
        for d in range(1, owners)
    ]
    for copy in got_ids:
        copy.start()
    for copy in got_ids:
        copy.wait()

    low_rows, high_rows = pl.ds(0, split), pl.ds(split, high - split)

    def add(where, value):
        part[where] = (part[where].astype(jnp.float32) + value.astype(jnp.float32)).astype(
            jnp.bfloat16
        )

    one = [
        send(part.at[far, :, :, low_rows], a_in, one_sem, 0, (g, far)),
        send(part.at[t, :, other, high_rows], b_in.at[0], one_sem, 1, (side, t)),
        send(part.at[far, :, other, high_rows], b_in.at[1], one_sem, 2, (side, t)),
    ]
    two = [
        send(part.at[t, :, other, low_rows], a2_in, two_sem, 0, (side, t)),
        send(part.at[far, :, x, high_rows], b2_in, two_sem, 1, (g, far)),
    ]
    last = [
        send(
            part.at[t, (z + d) % zs, x], z_in.at[d - 1], z_sem, d - 1, ((z + d) % zs * 2 + x, t)
        )
        for d in range(1, zs)
    ]

    def after_core():
        for copy in cross:
            copy.wait()
        for n, o in ((1, far), (0, t)):
            for k in range(zs):
                for j in range(2):
                    add((o, k, j), c_in[n, k, j])
        for copy in one:
            copy.start()

    def after_one():
        for copy in one:
            copy.wait()
        for k in range(zs):
            add((t, k, other, low_rows), a_in[k, other])
            add((far, k, x, high_rows), b_in[1, k])
        for copy in two:
            copy.start()
        for k in range(zs):
            add((t, k, x, low_rows), a_in[k, x])
            add((t, k, x, high_rows), b_in[0, k])

    def after_two():
        for copy in two:
            copy.wait()
        for k in range(zs):
            add((t, k, x, low_rows), a2_in[k])
            add((t, k, x, high_rows), b2_in[k])
        for copy in last:
            copy.start()

    stages = [after_core, after_one, after_two]
    returns = []
    wide[pl.ds(rows, 8), :] = jnp.zeros((8, width), jnp.float32)
    for s in range(slots):
        if s + 1 < slots:
            fetch(s + 1).start()
        fetch(s).wait()

        @pl.loop(0, rows // chunk)
        def _(c):
            at = pl.ds(pl.multiple_of(c * chunk, chunk), chunk)
            wide[at, :] = stage[s % 2, at, :].astype(jnp.float32)

        @pl.loop(0, owners * lines)
        def _(i):
            src = i // lines
            line = s * lines + i % lines
            for u in range(per_line):
                held = [
                    wide[pl.ds(idx_s[src, line, u * maxlen + k], 1), :] for k in range(maxlen)
                ]
                while len(held) > 1:
                    held = [a + b for a, b in zip(held[::2], held[1::2])] + (
                        [held[-1]] if len(held) % 2 else []
                    )
                acc[pl.ds(i * per_line + u, 1), :] = held[0]

        for n, at in enumerate(checkpoints):
            if at == s:
                stages[n]()
        got[t, s] = acc[pl.ds(pl.multiple_of(t * batch, batch), batch), :].astype(jnp.bfloat16)
        for d in range(1, owners):
            o = (t + d) % owners
            pooled[d - 1, s] = acc[pl.ds(pl.multiple_of(o * batch, batch), batch), :].astype(
                jnp.bfloat16
            )
            copy = send(
                pooled.at[d - 1, s], got.at[t, s], pool_sem, s * (owners - 1) + d - 1, (g, o)
            )
            copy.start()
            returns.append(copy)

    for copy in last:
        copy.wait()
    total = part[t, z, x].astype(jnp.float32)
    for d in range(1, zs):
        total += z_in[d - 1].astype(jnp.float32)
    grad_ref[...] = total
    for copy in returns:
        copy.wait()
    for f in range(slot_ref.shape[0]):
        s = slot_ref[f]
        emb_ref[:, f * width : (f + 1) * width] = got[lax.div(s, slots), lax.rem(s, slots)]


def fused_step(idx, slot_of_table, tables, cross_input, cotangent, up_weight, down_weight, maxlen, factor):
    groups, owners = lax.axis_size("grp"), lax.axis_size("tbl")
    slots, rows, width = tables.shape
    batch, depth = cross_input.shape
    zs, high = groups // 2, depth // groups
    split = (high // 2 + 15) // 16 * 16
    sems = pltpu.SemaphoreType.DMA
    bf16 = jnp.bfloat16
    vmem = pl.BlockSpec(memory_space=pltpu.VMEM)
    checkpoints = (0, min(3, slots - 1), min(5, slots - 1))
    return pl.pallas_call(
        functools.partial(step_kernel, maxlen, factor, split, checkpoints),
        out_shape=(
            jax.ShapeDtypeStruct((batch, slot_of_table.shape[0] * width), bf16),
            jax.ShapeDtypeStruct((high, LANES), jnp.float32),
        ),
        in_specs=[
            vmem,
            pl.BlockSpec(memory_space=pltpu.SMEM),
            pl.BlockSpec(memory_space=pl.ANY),
            vmem,
            vmem,
            vmem,
            vmem,
        ],
        out_specs=(vmem, vmem),
        scratch_shapes=[
            pltpu.VMEM(idx.shape, jnp.int32),
            pltpu.SMEM(idx.shape, jnp.int32),
            pltpu.VMEM((owners, zs, 2, high, LANES), bf16),
            pltpu.VMEM((2, zs, 2, high, LANES), bf16),
            pltpu.VMEM((zs, 2, split, LANES), bf16),
            pltpu.VMEM((2, zs, high - split, LANES), bf16),
            pltpu.VMEM((zs, split, LANES), bf16),
            pltpu.VMEM((zs, high - split, LANES), bf16),
            pltpu.VMEM((max(zs - 1, 1), high, LANES), bf16),
            pltpu.VMEM((2, rows, width), bf16),
            pltpu.VMEM((rows + 8, width), jnp.float32),
            pltpu.VMEM((owners * batch, width), jnp.float32),
            pltpu.VMEM((owners - 1, slots, batch, width), bf16),
            pltpu.VMEM((owners, slots, batch, width), bf16),
            sems((2,)),
            sems((owners,)),
            sems((2, owners - 1)),
            sems((2, 2)),
            sems((2, 3)),
            sems((2, 2)),
            sems((2, max(zs - 1, 1))),
            sems((2, slots * (owners - 1))),
        ],
        compiler_params=pltpu.CompilerParams(
            collective_id=0, has_side_effects=True, vmem_limit_bytes=56 << 20
        ),
        name="fused_step",
    )(idx, slot_of_table, tables, cross_input, cotangent, up_weight, down_weight)


def on_device(
    next_ids, next_lengths, slot_of_table, tables, cross_input, cotangent, up_weight, down_weight
):
    groups, owners = lax.axis_size("grp"), lax.axis_size("tbl")
    batch, depth = cross_input.shape
    rank = down_weight.shape[1]
    slots, rows, _ = tables.shape
    if owners != 4 or groups % 2 or depth % (16 * groups) or rank * 2 != owners * LANES:
        return plain(
            next_ids,
            next_lengths,
            slot_of_table,
            tables,
            cross_input,
            cotangent,
            up_weight,
            down_weight,
        )
    maxlen = next_ids.shape[1] // (slots * owners)
    factor = 1.0 / math.sqrt(batch * groups * owners)
    idx = bag_rows(next_ids, next_lengths, slot_of_table, slots, owners, rows)
    next_embedded, grads = fused_step(
        idx, slot_of_table, tables, cross_input, cotangent, up_weight, down_weight, maxlen, factor
    )
    half = LANES // 2
    return next_embedded, grads[:, :half].T, grads[:, half:]


def solution(mesh):
    return jax.shard_map(
        on_device,
        mesh=mesh,
        in_specs=(
            P(("grp", "tbl"), None),
            P(("grp", "tbl"), None),
            P(),
            P("tbl", None, None),
            P(("grp", "tbl"), None),
            P(("grp", "tbl"), None),
            P(),
            P(),
        ),
        out_specs=(P(("grp", "tbl"), None), P("tbl", "grp"), P("grp", "tbl")),
        check_vma=False,
    )
```

```python
import functools
import math

import jax
import jax.numpy as jnp
from jax import lax
from jax.experimental import pallas as pl
from jax.experimental.pallas import tpu as pltpu
from jax.sharding import PartitionSpec as P

LANES = 128


def pool_kernel(maxlen, idx_ref, tab_ref, out_ref, stage, wide, acc, sem):
    owners, batch, _ = out_ref.shape
    slots, rows, width = tab_ref.shape
    per_line = LANES // maxlen
    lines = batch // per_line
    chunk = 256

    def fetch(s):
        return pltpu.make_async_copy(tab_ref.at[s], stage.at[s % 2], sem.at[s % 2])

    fetch(0).start()
    wide[pl.ds(rows, 8), :] = jnp.zeros((8, width), jnp.float32)
    for s in range(slots):
        if s + 1 < slots:
            fetch(s + 1).start()
        fetch(s).wait()

        @pl.loop(0, rows // chunk)
        def _(c):
            at = pl.ds(pl.multiple_of(c * chunk, chunk), chunk)
            wide[at, :] = stage[s % 2, at, :].astype(jnp.float32)

        @pl.loop(0, owners * lines)
        def _(g):
            src = g // lines
            line = s * lines + g % lines
            for u in range(per_line):
                got = [
                    wide[pl.ds(idx_ref[src, line, u * maxlen + k], 1), :] for k in range(maxlen)
                ]
                while len(got) > 1:
                    got = [a + b for a, b in zip(got[::2], got[1::2])] + (
                        [got[-1]] if len(got) % 2 else []
                    )
                acc[pl.ds(g * per_line + u, 1), :] = got[0]

        for o in range(owners):
            out_ref[o, :, s * width : (s + 1) * width] = acc[
                o * batch : (o + 1) * batch, :
            ].astype(jnp.bfloat16)


def pool(idx, tables, batch, maxlen):
    slots, rows, width = tables.shape
    owners = idx.shape[0]
    return pl.pallas_call(
        functools.partial(pool_kernel, maxlen),
        out_shape=jax.ShapeDtypeStruct((owners, batch, slots * width), jnp.bfloat16),
        in_specs=[
            pl.BlockSpec(memory_space=pltpu.SMEM),
            pl.BlockSpec(memory_space=pl.ANY),
        ],
        out_specs=pl.BlockSpec(memory_space=pltpu.VMEM),
        scratch_shapes=[
            pltpu.VMEM((2, rows, width), jnp.bfloat16),
            pltpu.VMEM((rows + 8, width), jnp.float32),
            pltpu.VMEM((owners * batch, width), jnp.float32),
            pltpu.SemaphoreType.DMA((2,)),
        ],
        compiler_params=pltpu.CompilerParams(vmem_limit_bytes=60 << 20),
        cost_estimate=pl.CostEstimate(
            flops=100_000_000, bytes_accessed=tables.size * 2, transcendentals=0
        ),
        name="pool",
    )(idx, tables)


def order_kernel(slot_ref, got_ref, out_ref):
    owners, batch, wide = got_ref.shape
    feats = slot_ref.shape[0]
    width = out_ref.shape[1] // feats
    slots = wide // width
    for f in range(feats):
        s = slot_ref[f]
        at = pl.ds(pl.multiple_of(lax.rem(s, slots) * width, width), width)
        out_ref[:, f * width : (f + 1) * width] = got_ref[lax.div(s, slots), :, at]


def order(slot_of_table, got, width):
    return pl.pallas_call(
        order_kernel,
        out_shape=jax.ShapeDtypeStruct(
            (got.shape[1], slot_of_table.shape[0] * width), jnp.bfloat16
        ),
        in_specs=[
            pl.BlockSpec(memory_space=pltpu.SMEM),
            pl.BlockSpec(memory_space=pltpu.VMEM),
        ],
        out_specs=pl.BlockSpec(memory_space=pltpu.VMEM),
        name="order",
    )(slot_of_table, got)


def bag_rows(next_ids, next_lengths, slot_of_table, slots, owners, rows):
    batch = next_ids.shape[0]
    slots_all = slots * owners
    maxlen = next_ids.shape[1] // slots_all
    hit = (slot_of_table[:, None] == lax.broadcasted_iota(jnp.int32, (1, slots_all), 1)).astype(
        jnp.int32
    )
    slot_lengths = jnp.sum(next_lengths[:, :, None] * hit[None, :, :], axis=1)
    keep = lax.broadcasted_iota(jnp.int32, (batch, slots_all, maxlen), 2) < slot_lengths[:, :, None]
    idx = jnp.where(keep, next_ids.reshape(batch, slots_all, maxlen), rows)
    return idx.transpose(1, 0, 2).reshape(owners, slots * batch * maxlen // LANES, LANES)


def plain(
    next_ids, next_lengths, slot_of_table, tables, cross_input, cotangent, up_weight, down_weight
):
    batch = next_ids.shape[0]
    owners = lax.axis_size("tbl")
    slots, rows, width = tables.shape
    maxlen = next_ids.shape[1] // (slots * owners)
    idx = bag_rows(next_ids, next_lengths, slot_of_table, slots, owners, rows)
    low = jnp.dot(cross_input, down_weight, preferred_element_type=jnp.float32).astype(jnp.bfloat16)
    dz = (cotangent.astype(jnp.float32) * cross_input.astype(jnp.float32)).astype(jnp.bfloat16)
    dlow = jnp.dot(dz, up_weight.T, preferred_element_type=jnp.float32).astype(jnp.bfloat16)
    total = batch * lax.axis_size("grp") * owners
    factor = 1.0 / math.sqrt(total)
    part_up = jnp.dot(low.T, dz, preferred_element_type=jnp.float32) * factor
    part_down = jnp.dot(cross_input.T, dlow, preferred_element_type=jnp.float32) * factor
    part_up, part_down = part_up.astype(jnp.bfloat16), part_down.astype(jnp.bfloat16)
    owner_up, owner_down = (
        lax.psum_scatter(part_up, "tbl", scatter_dimension=0, tiled=True).astype(jnp.float32),
        lax.psum_scatter(part_down, "tbl", scatter_dimension=1, tiled=True).astype(jnp.float32),
    )
    got_idx = lax.all_to_all(idx, "tbl", split_axis=0, concat_axis=0, tiled=True)
    pooled = pool(got_idx, tables, batch, maxlen)
    returned = lax.all_to_all(pooled, "tbl", split_axis=0, concat_axis=0, tiled=True)
    next_embedded = order(slot_of_table, returned, width)
    grad_up, grad_down = (
        lax.psum_scatter(owner_up, "grp", scatter_dimension=1, tiled=True),
        lax.psum_scatter(owner_down, "grp", scatter_dimension=0, tiled=True),
    )
    return (next_embedded, grad_up, grad_down)


def step_kernel(
    maxlen,
    factor,
    split,
    checkpoints,
    ids_ref,
    len_ref,
    slot_ref,
    tab_ref,
    x_hbm,
    ct_hbm,
    up_hbm,
    down_hbm,
    emb_ref,
    grad_up_ref,
    grad_down_ref,
    x_ref,
    ct_ref,
    up_ref,
    down_ref,
    idx_ref,
    idx_in,
    idx_s,
    part,
    c_in,
    a_in,
    b_in,
    a2_in,
    b2_in,
    z_in,
    stage,
    wide,
    acc,
    pooled,
    got,
    tab_sem,
    smem_sem,
    idx_sem,
    core_sem,
    one_sem,
    two_sem,
    z_sem,
    pool_sem,
    load_sem,
):
    owners, zs, _, high, lanes = part.shape
    slots, rows, width = tab_ref.shape
    batch = x_ref.shape[0]
    rank = down_ref.shape[1]
    cols = rank // owners
    group = 16
    chunk = 256
    g, t = lax.axis_index("grp"), lax.axis_index("tbl")
    z, x = g // 2, g % 2
    core = t + 1 - 2 * (t % 2)
    far = (t + 2) % owners
    other = 1 - x
    side = g + 1 - 2 * x

    def fetch(s):
        return pltpu.make_async_copy(tab_ref.at[s], stage.at[s % 2], tab_sem.at[s % 2])

    def send(src, dst, sems, n, device):
        return pltpu.make_async_remote_copy(
            src_ref=src,
            dst_ref=dst,
            send_sem=sems.at[0, n],
            recv_sem=sems.at[1, n],
            device_id=device,
            device_id_type=pl.DeviceIdType.MESH,
        )

    loads = [
        pltpu.make_async_copy(a, b, load_sem.at[n])
        for n, (a, b) in enumerate(
            ((x_hbm, x_ref), (down_hbm, down_ref), (ct_hbm, ct_ref), (up_hbm, up_ref))
        )
    ]
    for copy in loads:
        copy.start()
    fetch(0).start()
    barrier = pltpu.get_barrier_semaphore()
    near = [(g, (t + d) % owners) for d in range(1, owners)] + [(side, t)]
    near += [((z + d) % zs * 2 + x, t) for d in range(1, zs)]
    for device in near:
        pl.semaphore_signal(
            barrier, inc=1, device_id=device, device_id_type=pl.DeviceIdType.MESH
        )

    feats, span = slot_ref.shape[0], ids_ref.shape[0]
    each = slots * maxlen
    feat = lax.broadcasted_iota(jnp.int32, (span, feats), 1)
    entry = lax.broadcasted_iota(jnp.int32, (span, feats), 0)
    held_by = jnp.zeros((span, feats), jnp.int32)
    for f in range(feats):
        held_by = jnp.where(feat == f, slot_ref[f], held_by)
    hit = jnp.where(held_by == entry // maxlen, 1.0, 0.0).astype(jnp.bfloat16)
    lens = jnp.dot(
        hit, len_ref[...].astype(jnp.float32).astype(jnp.bfloat16), preferred_element_type=jnp.float32
    )
    place = (lax.broadcasted_iota(jnp.int32, (span, batch), 0) % maxlen).astype(jnp.float32)
    idx = jnp.where(place < lens, ids_ref[...], rows)
    for o in range(owners):
        idx_ref[o] = idx[o * each : (o + 1) * each]

    pl.semaphore_wait(barrier, len(near))

    ids_out = [
        send(idx_ref.at[(t + d) % owners], idx_in.at[t], idx_sem, d - 1, (g, (t + d) % owners))
        for d in range(1, owners)
    ]
    for copy in ids_out:
        copy.start()
    keep_ids = pltpu.make_async_copy(idx_ref.at[t], idx_s.at[t], smem_sem.at[0])
    keep_ids.start()

    loads[0].wait()
    loads[1].wait()
    low = jnp.dot(x_ref[...], down_ref[...], preferred_element_type=jnp.float32).astype(jnp.bfloat16)
    loads[2].wait()
    dz = (ct_ref[...].astype(jnp.float32) * x_ref[...].astype(jnp.float32)).astype(jnp.bfloat16)
    loads[3].wait()
    dlow = lax.dot_general(
        dz, up_ref[...], (((1,), (1,)), ((), ())), preferred_element_type=jnp.float32
    ).astype(jnp.bfloat16)
    first = (((0,), (0,)), ((), ()))
    for block in range(2 * zs):
        begin = block * high
        edge = begin // LANES * LANES
        stop = -(-(begin + high) // LANES) * LANES
        up = lax.dot_general(dz[:, edge:stop], low, first, preferred_element_type=jnp.float32)
        down = lax.dot_general(
            x_ref[:, edge:stop], dlow, first, preferred_element_type=jnp.float32
        )
        up = (up[begin - edge : begin - edge + high] * factor).astype(jnp.bfloat16)
        down = (down[begin - edge : begin - edge + high] * factor).astype(jnp.bfloat16)
        for o in range(owners):
            part[o, block // 2, block % 2] = jnp.concatenate(
                [up[:, o * cols : (o + 1) * cols], down[:, o * cols : (o + 1) * cols]], axis=1
            )

    cross = [
        send(part.at[core], c_in.at[0], core_sem, 0, (g, core)),
        send(part.at[(core + 2) % owners], c_in.at[1], core_sem, 1, (g, core)),
    ]
    for copy in cross:
        copy.start()

    for copy in ids_out:
        copy.wait()
    keep_ids.wait()
    got_ids = [
        pltpu.make_async_copy(
            idx_in.at[(t + d) % owners], idx_s.at[(t + d) % owners], smem_sem.at[d]
        )
        for d in range(1, owners)
    ]
    for copy in got_ids:
        copy.start()
    for copy in got_ids:
        copy.wait()

    low_rows, high_rows = pl.ds(0, split), pl.ds(split, high - split)

    def add(where, value):
        part[where] = (part[where].astype(jnp.float32) + value.astype(jnp.float32)).astype(
            jnp.bfloat16
        )

    one = [
        send(part.at[far, :, :, low_rows], a_in, one_sem, 0, (g, far)),
        send(part.at[t, :, other, high_rows], b_in.at[0], one_sem, 1, (side, t)),
        send(part.at[far, :, other, high_rows], b_in.at[1], one_sem, 2, (side, t)),
    ]
    two = [
        send(part.at[t, :, other, low_rows], a2_in, two_sem, 0, (side, t)),
        send(part.at[far, :, x, high_rows], b2_in, two_sem, 1, (g, far)),
    ]
    last = [
        send(
            part.at[t, (z + d) % zs, x], z_in.at[d - 1], z_sem, d - 1, ((z + d) % zs * 2 + x, t)
        )
        for d in range(1, zs)
    ]

    def after_core():
        for copy in cross:
            copy.wait()
        for n, o in ((1, far), (0, t)):
            for k in range(zs):
                for j in range(2):
                    add((o, k, j), c_in[n, k, j])
        for copy in one:
            copy.start()

    def after_one():
        for copy in one:
            copy.wait()
        for k in range(zs):
            add((t, k, other, low_rows), a_in[k, other])
            add((far, k, x, high_rows), b_in[1, k])
        for copy in two:
            copy.start()
        for k in range(zs):
            add((t, k, x, low_rows), a_in[k, x])
            add((t, k, x, high_rows), b_in[0, k])

    def after_two():
        for copy in two:
            copy.wait()
        for k in range(zs):
            add((t, k, x, low_rows), a2_in[k])
            add((t, k, x, high_rows), b2_in[k])
        for copy in last:
            copy.start()

    stages = [after_core, after_one, after_two]
    returns = []
    wide[pl.ds(rows, 8), :] = jnp.zeros((8, width), jnp.float32)
    for s in range(slots):
        if s + 1 < slots:
            fetch(s + 1).start()
        fetch(s).wait()

        @pl.loop(0, rows // chunk)
        def _(c):
            at = pl.ds(pl.multiple_of(c * chunk, chunk), chunk)
            wide[at, :] = stage[s % 2, at, :].astype(jnp.float32)

        @pl.loop(0, owners * batch // group)
        def _(i):
            src = i // (batch // group)
            line = i % (batch // group) * group
            for u in range(group):
                held = [
                    wide[pl.ds(idx_s[src, s * maxlen + k, line + u], 1), :] for k in range(maxlen)
                ]
                while len(held) > 1:
                    held = [a + b for a, b in zip(held[::2], held[1::2])] + (
                        [held[-1]] if len(held) % 2 else []
                    )
                acc[pl.ds(i * group + u, 1), :] = held[0]

        for n, at in enumerate(checkpoints):
            if at == s:
                stages[n]()
        got[t, s] = acc[pl.ds(pl.multiple_of(t * batch, batch), batch), :].astype(jnp.bfloat16)
        for d in range(1, owners):
            o = (t + d) % owners
            pooled[d - 1, s] = acc[pl.ds(pl.multiple_of(o * batch, batch), batch), :].astype(
                jnp.bfloat16
            )
            copy = send(
                pooled.at[d - 1, s], got.at[t, s], pool_sem, s * (owners - 1) + d - 1, (g, o)
            )
            copy.start()
            returns.append(copy)

    for copy in last:
        copy.wait()
    total = part[t, z, x].astype(jnp.float32)
    for d in range(1, zs):
        total += z_in[d - 1].astype(jnp.float32)
    total = total.T
    grad_up_ref[...] = total[:cols]
    grad_down_ref[...] = total[cols:]
    for copy in returns:
        copy.wait()
    for f in range(slot_ref.shape[0]):
        s = slot_ref[f]
        emb_ref[:, f * width : (f + 1) * width] = got[lax.div(s, slots), lax.rem(s, slots)]


def fused_step(
    next_ids, next_lengths, slot_of_table, tables, cross_input, cotangent, up_weight, down_weight, maxlen, factor
):
    groups, owners = lax.axis_size("grp"), lax.axis_size("tbl")
    slots, rows, width = tables.shape
    batch, depth = cross_input.shape
    zs, high = groups // 2, depth // groups
    split = (high // 2 + 15) // 16 * 16
    sems = pltpu.SemaphoreType.DMA
    bf16 = jnp.bfloat16
    any_space = pl.BlockSpec(memory_space=pl.ANY)
    idx_shape = (owners, next_ids.shape[1] // owners, batch)
    half = down_weight.shape[1] // owners
    vmem = pl.BlockSpec(memory_space=pltpu.VMEM)
    checkpoints = (0, min(3, slots - 1), min(5, slots - 1))
    return pl.pallas_call(
        functools.partial(step_kernel, maxlen, factor, split, checkpoints),
        out_shape=(
            jax.ShapeDtypeStruct((batch, slot_of_table.shape[0] * width), bf16),
            jax.ShapeDtypeStruct((half, high), jnp.float32),
            jax.ShapeDtypeStruct((half, high), jnp.float32),
        ),
        in_specs=[
            vmem,
            vmem,
            pl.BlockSpec(memory_space=pltpu.SMEM),
            any_space,
            any_space,
            any_space,
            any_space,
            any_space,
        ],
        out_specs=(vmem, vmem, vmem),
        scratch_shapes=[
            pltpu.VMEM(cross_input.shape, bf16),
            pltpu.VMEM(cotangent.shape, bf16),
            pltpu.VMEM(up_weight.shape, bf16),
            pltpu.VMEM(down_weight.shape, bf16),
            pltpu.VMEM(idx_shape, jnp.int32),
            pltpu.VMEM(idx_shape, jnp.int32),
            pltpu.SMEM(idx_shape, jnp.int32),
            pltpu.VMEM((owners, zs, 2, high, LANES), bf16),
            pltpu.VMEM((2, zs, 2, high, LANES), bf16),
            pltpu.VMEM((zs, 2, split, LANES), bf16),
            pltpu.VMEM((2, zs, high - split, LANES), bf16),
            pltpu.VMEM((zs, split, LANES), bf16),
            pltpu.VMEM((zs, high - split, LANES), bf16),
            pltpu.VMEM((max(zs - 1, 1), high, LANES), bf16),
            pltpu.VMEM((2, rows, width), bf16),
            pltpu.VMEM((rows + 8, width), jnp.float32),
            pltpu.VMEM((owners * batch, width), jnp.float32),
            pltpu.VMEM((owners - 1, slots, batch, width), bf16),
            pltpu.VMEM((owners, slots, batch, width), bf16),
            sems((2,)),
            sems((owners,)),
            sems((2, owners - 1)),
            sems((2, 2)),
            sems((2, 3)),
            sems((2, 2)),
            sems((2, max(zs - 1, 1))),
            sems((2, slots * (owners - 1))),
            sems((4,)),
        ],
        compiler_params=pltpu.CompilerParams(
            collective_id=0, has_side_effects=True, vmem_limit_bytes=56 << 20
        ),
        name="fused_step",
    )(
        next_ids.T,
        next_lengths.T,
        slot_of_table,
        tables,
        cross_input,
        cotangent,
        up_weight,
        down_weight,
    )


def on_device(
    next_ids, next_lengths, slot_of_table, tables, cross_input, cotangent, up_weight, down_weight
):
    groups, owners = lax.axis_size("grp"), lax.axis_size("tbl")
    batch, depth = cross_input.shape
    rank = down_weight.shape[1]
    slots, rows, _ = tables.shape
    maxlen = next_ids.shape[1] // (slots * owners)
    fits = owners == 4 and groups % 2 == 0 and depth % (16 * groups) == 0 and batch % 16 == 0
    if not fits or rank * 2 != owners * LANES or slots * maxlen % 8 or batch != LANES:
        return plain(
            next_ids,
            next_lengths,
            slot_of_table,
            tables,
            cross_input,
            cotangent,
            up_weight,
            down_weight,
        )
    factor = 1.0 / math.sqrt(batch * groups * owners)
    next_embedded, grad_up, grad_down = fused_step(
        next_ids,
        next_lengths,
        slot_of_table,
        tables,
        cross_input,
        cotangent,
        up_weight,
        down_weight,
        maxlen,
        factor,
    )
    return next_embedded, grad_up, grad_down.T


def solution(mesh):
    return jax.shard_map(
        on_device,
        mesh=mesh,
        in_specs=(
            P(("grp", "tbl"), None),
            P(("grp", "tbl"), None),
            P(),
            P("tbl", None, None),
            P(("grp", "tbl"), None),
            P(("grp", "tbl"), None),
            P(),
            P(),
        ),
        out_specs=(P(("grp", "tbl"), None), P("tbl", "grp"), P("grp", "tbl")),
        check_vma=False,
    )
```

```python
import functools
import math

import jax
import jax.numpy as jnp
from jax import lax
from jax.experimental import pallas as pl
from jax.experimental.pallas import tpu as pltpu
from jax.sharding import PartitionSpec as P

LANES = 128


def pool_kernel(maxlen, idx_ref, tab_ref, out_ref, stage, wide, acc, sem):
    owners, batch, _ = out_ref.shape
    slots, rows, width = tab_ref.shape
    per_line = LANES // maxlen
    lines = batch // per_line
    chunk = 256

    def fetch(s):
        return pltpu.make_async_copy(tab_ref.at[s], stage.at[s % 2], sem.at[s % 2])

    fetch(0).start()
    wide[pl.ds(rows, 8), :] = jnp.zeros((8, width), jnp.float32)
    for s in range(slots):
        if s + 1 < slots:
            fetch(s + 1).start()
        fetch(s).wait()

        @pl.loop(0, rows // chunk)
        def _(c):
            at = pl.ds(pl.multiple_of(c * chunk, chunk), chunk)
            wide[at, :] = stage[s % 2, at, :].astype(jnp.float32)

        @pl.loop(0, owners * lines)
        def _(g):
            src = g // lines
            line = s * lines + g % lines
            for u in range(per_line):
                got = [
                    wide[pl.ds(idx_ref[src, line, u * maxlen + k], 1), :] for k in range(maxlen)
                ]
                while len(got) > 1:
                    got = [a + b for a, b in zip(got[::2], got[1::2])] + (
                        [got[-1]] if len(got) % 2 else []
                    )
                acc[pl.ds(g * per_line + u, 1), :] = got[0]

        for o in range(owners):
            out_ref[o, :, s * width : (s + 1) * width] = acc[
                o * batch : (o + 1) * batch, :
            ].astype(jnp.bfloat16)


def pool(idx, tables, batch, maxlen):
    slots, rows, width = tables.shape
    owners = idx.shape[0]
    return pl.pallas_call(
        functools.partial(pool_kernel, maxlen),
        out_shape=jax.ShapeDtypeStruct((owners, batch, slots * width), jnp.bfloat16),
        in_specs=[
            pl.BlockSpec(memory_space=pltpu.SMEM),
            pl.BlockSpec(memory_space=pl.ANY),
        ],
        out_specs=pl.BlockSpec(memory_space=pltpu.VMEM),
        scratch_shapes=[
            pltpu.VMEM((2, rows, width), jnp.bfloat16),
            pltpu.VMEM((rows + 8, width), jnp.float32),
            pltpu.VMEM((owners * batch, width), jnp.float32),
            pltpu.SemaphoreType.DMA((2,)),
        ],
        compiler_params=pltpu.CompilerParams(vmem_limit_bytes=60 << 20),
        cost_estimate=pl.CostEstimate(
            flops=100_000_000, bytes_accessed=tables.size * 2, transcendentals=0
        ),
        name="pool",
    )(idx, tables)


def order_kernel(slot_ref, got_ref, out_ref):
    owners, batch, wide = got_ref.shape
    feats = slot_ref.shape[0]
    width = out_ref.shape[1] // feats
    slots = wide // width
    for f in range(feats):
        s = slot_ref[f]
        at = pl.ds(pl.multiple_of(lax.rem(s, slots) * width, width), width)
        out_ref[:, f * width : (f + 1) * width] = got_ref[lax.div(s, slots), :, at]


def order(slot_of_table, got, width):
    return pl.pallas_call(
        order_kernel,
        out_shape=jax.ShapeDtypeStruct(
            (got.shape[1], slot_of_table.shape[0] * width), jnp.bfloat16
        ),
        in_specs=[
            pl.BlockSpec(memory_space=pltpu.SMEM),
            pl.BlockSpec(memory_space=pltpu.VMEM),
        ],
        out_specs=pl.BlockSpec(memory_space=pltpu.VMEM),
        name="order",
    )(slot_of_table, got)


def bag_rows(next_ids, next_lengths, slot_of_table, slots, owners, rows):
    batch = next_ids.shape[0]
    slots_all = slots * owners
    maxlen = next_ids.shape[1] // slots_all
    hit = (slot_of_table[:, None] == lax.broadcasted_iota(jnp.int32, (1, slots_all), 1)).astype(
        jnp.int32
    )
    slot_lengths = jnp.sum(next_lengths[:, :, None] * hit[None, :, :], axis=1)
    keep = lax.broadcasted_iota(jnp.int32, (batch, slots_all, maxlen), 2) < slot_lengths[:, :, None]
    idx = jnp.where(keep, next_ids.reshape(batch, slots_all, maxlen), rows)
    return idx.transpose(1, 0, 2).reshape(owners, slots * batch * maxlen // LANES, LANES)


def plain(
    next_ids, next_lengths, slot_of_table, tables, cross_input, cotangent, up_weight, down_weight
):
    batch = next_ids.shape[0]
    owners = lax.axis_size("tbl")
    slots, rows, width = tables.shape
    maxlen = next_ids.shape[1] // (slots * owners)
    idx = bag_rows(next_ids, next_lengths, slot_of_table, slots, owners, rows)
    low = jnp.dot(cross_input, down_weight, preferred_element_type=jnp.float32).astype(jnp.bfloat16)
    dz = (cotangent.astype(jnp.float32) * cross_input.astype(jnp.float32)).astype(jnp.bfloat16)
    dlow = jnp.dot(dz, up_weight.T, preferred_element_type=jnp.float32).astype(jnp.bfloat16)
    total = batch * lax.axis_size("grp") * owners
    factor = 1.0 / math.sqrt(total)
    part_up = jnp.dot(low.T, dz, preferred_element_type=jnp.float32) * factor
    part_down = jnp.dot(cross_input.T, dlow, preferred_element_type=jnp.float32) * factor
    part_up, part_down = part_up.astype(jnp.bfloat16), part_down.astype(jnp.bfloat16)
    owner_up, owner_down = (
        lax.psum_scatter(part_up, "tbl", scatter_dimension=0, tiled=True).astype(jnp.float32),
        lax.psum_scatter(part_down, "tbl", scatter_dimension=1, tiled=True).astype(jnp.float32),
    )
    got_idx = lax.all_to_all(idx, "tbl", split_axis=0, concat_axis=0, tiled=True)
    pooled = pool(got_idx, tables, batch, maxlen)
    returned = lax.all_to_all(pooled, "tbl", split_axis=0, concat_axis=0, tiled=True)
    next_embedded = order(slot_of_table, returned, width)
    grad_up, grad_down = (
        lax.psum_scatter(owner_up, "grp", scatter_dimension=1, tiled=True),
        lax.psum_scatter(owner_down, "grp", scatter_dimension=0, tiled=True),
    )
    return (next_embedded, grad_up, grad_down)


def step_kernel(
    maxlen,
    factor,
    split,
    checkpoints,
    ids_ref,
    len_ref,
    slot_ref,
    tab_ref,
    x_hbm,
    ct_hbm,
    up_hbm,
    down_hbm,
    emb_ref,
    grad_up_ref,
    grad_down_ref,
    x_ref,
    ct_ref,
    up_ref,
    down_ref,
    idx_ref,
    idx_in,
    turned,
    idx_s,
    part,
    c_in,
    a_in,
    b_in,
    a2_in,
    b2_in,
    z_in,
    stage,
    wide,
    acc,
    pooled,
    got,
    tab_sem,
    smem_sem,
    idx_sem,
    core_sem,
    one_sem,
    two_sem,
    z_sem,
    pool_sem,
    load_sem,
):
    owners, zs, _, high, lanes = part.shape
    slots, rows, width = tab_ref.shape
    batch = x_ref.shape[0]
    rank = down_ref.shape[1]
    cols = rank // owners
    group = 16
    chunk = 256
    g, t = lax.axis_index("grp"), lax.axis_index("tbl")
    z, x = g // 2, g % 2
    core = t + 1 - 2 * (t % 2)
    far = (t + 2) % owners
    other = 1 - x
    side = g + 1 - 2 * x

    def fetch(s):
        return pltpu.make_async_copy(tab_ref.at[s], stage.at[s % 2], tab_sem.at[s % 2])

    def send(src, dst, sems, n, device):
        return pltpu.make_async_remote_copy(
            src_ref=src,
            dst_ref=dst,
            send_sem=sems.at[0, n],
            recv_sem=sems.at[1, n],
            device_id=device,
            device_id_type=pl.DeviceIdType.MESH,
        )

    loads = [
        pltpu.make_async_copy(a, b, load_sem.at[n])
        for n, (a, b) in enumerate(
            ((x_hbm, x_ref), (down_hbm, down_ref), (ct_hbm, ct_ref), (up_hbm, up_ref))
        )
    ]
    for copy in loads:
        copy.start()
    fetch(0).start()
    barrier = pltpu.get_barrier_semaphore()
    near = [(g, (t + d) % owners) for d in range(1, owners)] + [(side, t)]
    near += [((z + d) % zs * 2 + x, t) for d in range(1, zs)]
    for device in near:
        pl.semaphore_signal(
            barrier, inc=1, device_id=device, device_id_type=pl.DeviceIdType.MESH
        )

    feats, span = slot_ref.shape[0], ids_ref.shape[0]
    each = slots * maxlen
    feat = lax.broadcasted_iota(jnp.int32, (span, feats), 1)
    entry = lax.broadcasted_iota(jnp.int32, (span, feats), 0)
    held_by = jnp.zeros((span, feats), jnp.int32)
    for f in range(feats):
        held_by = jnp.where(feat == f, slot_ref[f], held_by)
    hit = jnp.where(held_by == entry // maxlen, 1.0, 0.0).astype(jnp.bfloat16)
    lens = jnp.dot(
        hit, len_ref[...].astype(jnp.float32).astype(jnp.bfloat16), preferred_element_type=jnp.float32
    )
    place = (lax.broadcasted_iota(jnp.int32, (span, batch), 0) % maxlen).astype(jnp.float32)
    idx = jnp.where(place < lens, ids_ref[...], rows)
    for o in range(owners):
        idx_ref[o] = idx[o * each : (o + 1) * each]

    pl.semaphore_wait(barrier, len(near))

    ids_out = [
        send(idx_ref.at[(t + d) % owners], idx_in.at[t], idx_sem, d - 1, (g, (t + d) % owners))
        for d in range(1, owners)
    ]
    for copy in ids_out:
        copy.start()

    loads[0].wait()
    loads[1].wait()
    low = jnp.dot(x_ref[...], down_ref[...], preferred_element_type=jnp.float32).astype(jnp.bfloat16)
    loads[2].wait()
    dz = (ct_ref[...].astype(jnp.float32) * x_ref[...].astype(jnp.float32)).astype(jnp.bfloat16)
    loads[3].wait()
    dlow = lax.dot_general(
        dz, up_ref[...], (((1,), (1,)), ((), ())), preferred_element_type=jnp.float32
    ).astype(jnp.bfloat16)
    first = (((0,), (0,)), ((), ()))
    for block in range(2 * zs):
        begin = block * high
        edge = begin // LANES * LANES
        stop = -(-(begin + high) // LANES) * LANES
        up = lax.dot_general(dz[:, edge:stop], low, first, preferred_element_type=jnp.float32)
        down = lax.dot_general(
            x_ref[:, edge:stop], dlow, first, preferred_element_type=jnp.float32
        )
        up = (up[begin - edge : begin - edge + high] * factor).astype(jnp.bfloat16)
        down = (down[begin - edge : begin - edge + high] * factor).astype(jnp.bfloat16)
        for o in range(owners):
            part[o, block // 2, block % 2] = jnp.concatenate(
                [up[:, o * cols : (o + 1) * cols], down[:, o * cols : (o + 1) * cols]], axis=1
            )

    cross = [
        send(part.at[core], c_in.at[0], core_sem, 0, (g, core)),
        send(part.at[(core + 2) % owners], c_in.at[1], core_sem, 1, (g, core)),
    ]
    for copy in cross:
        copy.start()

    for copy in ids_out:
        copy.wait()
    idx_in[t] = idx_ref[t]
    for o in range(owners):
        turned[o] = jnp.zeros((batch, LANES), jnp.int32)
        turned[o, :, :each] = idx_in[o].T
    got_ids = [
        pltpu.make_async_copy(turned.at[o], idx_s.at[o], smem_sem.at[o]) for o in range(owners)
    ]
    for copy in got_ids:
        copy.start()
    for copy in got_ids:
        copy.wait()

    low_rows, high_rows = pl.ds(0, split), pl.ds(split, high - split)

    def add(where, value):
        part[where] = (part[where].astype(jnp.float32) + value.astype(jnp.float32)).astype(
            jnp.bfloat16
        )

    one = [
        send(part.at[far, :, :, low_rows], a_in, one_sem, 0, (g, far)),
        send(part.at[t, :, other, high_rows], b_in.at[0], one_sem, 1, (side, t)),
        send(part.at[far, :, other, high_rows], b_in.at[1], one_sem, 2, (side, t)),
    ]
    two = [
        send(part.at[t, :, other, low_rows], a2_in, two_sem, 0, (side, t)),
        send(part.at[far, :, x, high_rows], b2_in, two_sem, 1, (g, far)),
    ]
    last = [
        send(
            part.at[t, (z + d) % zs, x], z_in.at[d - 1], z_sem, d - 1, ((z + d) % zs * 2 + x, t)
        )
        for d in range(1, zs)
    ]

    def after_core():
        for copy in cross:
            copy.wait()
        for n, o in ((1, far), (0, t)):
            for k in range(zs):
                for j in range(2):
                    add((o, k, j), c_in[n, k, j])
        for copy in one:
            copy.start()

    def after_one():
        for copy in one:
            copy.wait()
        for k in range(zs):
            add((t, k, other, low_rows), a_in[k, other])
            add((far, k, x, high_rows), b_in[1, k])
        for copy in two:
            copy.start()
        for k in range(zs):
            add((t, k, x, low_rows), a_in[k, x])
            add((t, k, x, high_rows), b_in[0, k])

    def after_two():
        for copy in two:
            copy.wait()
        for k in range(zs):
            add((t, k, x, low_rows), a2_in[k])
            add((t, k, x, high_rows), b2_in[k])
        for copy in last:
            copy.start()

    stages = [after_core, after_one, after_two]
    returns = []
    wide[pl.ds(rows, 8), :] = jnp.zeros((8, width), jnp.float32)
    for s in range(slots):
        if s + 1 < slots:
            fetch(s + 1).start()
        fetch(s).wait()

        @pl.loop(0, rows // chunk)
        def _(c):
            at = pl.ds(pl.multiple_of(c * chunk, chunk), chunk)
            wide[at, :] = stage[s % 2, at, :].astype(jnp.float32)

        @pl.loop(0, owners * batch // group)
        def _(i):
            src = i // (batch // group)
            line = i % (batch // group) * group
            for u in range(group):
                held = [
                    wide[pl.ds(idx_s[src, line + u, s * maxlen + k], 1), :] for k in range(maxlen)
                ]
                while len(held) > 1:
                    held = [a + b for a, b in zip(held[::2], held[1::2])] + (
                        [held[-1]] if len(held) % 2 else []
                    )
                acc[pl.ds(i * group + u, 1), :] = held[0]

        for n, at in enumerate(checkpoints):
            if at == s:
                stages[n]()
        got[t, s] = acc[pl.ds(pl.multiple_of(t * batch, batch), batch), :].astype(jnp.bfloat16)
        for d in range(1, owners):
            o = (t + d) % owners
            pooled[d - 1, s] = acc[pl.ds(pl.multiple_of(o * batch, batch), batch), :].astype(
                jnp.bfloat16
            )
            copy = send(
                pooled.at[d - 1, s], got.at[t, s], pool_sem, s * (owners - 1) + d - 1, (g, o)
            )
            copy.start()
            returns.append(copy)

    for copy in last:
        copy.wait()
    total = part[t, z, x].astype(jnp.float32)
    for d in range(1, zs):
        total += z_in[d - 1].astype(jnp.float32)
    total = total.T
    grad_up_ref[...] = total[:cols]
    grad_down_ref[...] = total[cols:]
    for copy in returns:
        copy.wait()
    for f in range(slot_ref.shape[0]):
        s = slot_ref[f]
        emb_ref[:, f * width : (f + 1) * width] = got[lax.div(s, slots), lax.rem(s, slots)]


def fused_step(
    next_ids, next_lengths, slot_of_table, tables, cross_input, cotangent, up_weight, down_weight, maxlen, factor
):
    groups, owners = lax.axis_size("grp"), lax.axis_size("tbl")
    slots, rows, width = tables.shape
    batch, depth = cross_input.shape
    zs, high = groups // 2, depth // groups
    split = (high // 2 + 15) // 16 * 16
    sems = pltpu.SemaphoreType.DMA
    bf16 = jnp.bfloat16
    any_space = pl.BlockSpec(memory_space=pl.ANY)
    idx_shape = (owners, next_ids.shape[1] // owners, batch)
    half = down_weight.shape[1] // owners
    vmem = pl.BlockSpec(memory_space=pltpu.VMEM)
    checkpoints = (0, min(3, slots - 1), min(5, slots - 1))
    return pl.pallas_call(
        functools.partial(step_kernel, maxlen, factor, split, checkpoints),
        out_shape=(
            jax.ShapeDtypeStruct((batch, slot_of_table.shape[0] * width), bf16),
            jax.ShapeDtypeStruct((half, high), jnp.float32),
            jax.ShapeDtypeStruct((half, high), jnp.float32),
        ),
        in_specs=[
            vmem,
            vmem,
            pl.BlockSpec(memory_space=pltpu.SMEM),
            any_space,
            any_space,
            any_space,
            any_space,
            any_space,
        ],
        out_specs=(vmem, vmem, vmem),
        scratch_shapes=[
            pltpu.VMEM(cross_input.shape, bf16),
            pltpu.VMEM(cotangent.shape, bf16),
            pltpu.VMEM(up_weight.shape, bf16),
            pltpu.VMEM(down_weight.shape, bf16),
            pltpu.VMEM(idx_shape, jnp.int32),
            pltpu.VMEM(idx_shape, jnp.int32),
            pltpu.VMEM((owners, batch, LANES), jnp.int32),
            pltpu.SMEM((owners, batch, LANES), jnp.int32),
            pltpu.VMEM((owners, zs, 2, high, LANES), bf16),
            pltpu.VMEM((2, zs, 2, high, LANES), bf16),
            pltpu.VMEM((zs, 2, split, LANES), bf16),
            pltpu.VMEM((2, zs, high - split, LANES), bf16),
            pltpu.VMEM((zs, split, LANES), bf16),
            pltpu.VMEM((zs, high - split, LANES), bf16),
            pltpu.VMEM((max(zs - 1, 1), high, LANES), bf16),
            pltpu.VMEM((2, rows, width), bf16),
            pltpu.VMEM((rows + 8, width), jnp.float32),
            pltpu.VMEM((owners * batch, width), jnp.float32),
            pltpu.VMEM((owners - 1, slots, batch, width), bf16),
            pltpu.VMEM((owners, slots, batch, width), bf16),
            sems((2,)),
            sems((owners,)),
            sems((2, owners - 1)),
            sems((2, 2)),
            sems((2, 3)),
            sems((2, 2)),
            sems((2, max(zs - 1, 1))),
            sems((2, slots * (owners - 1))),
            sems((4,)),
        ],
        compiler_params=pltpu.CompilerParams(
            collective_id=0, has_side_effects=True, vmem_limit_bytes=56 << 20
        ),
        name="fused_step",
    )(
        next_ids.T,
        next_lengths.T,
        slot_of_table,
        tables,
        cross_input,
        cotangent,
        up_weight,
        down_weight,
    )


def on_device(
    next_ids, next_lengths, slot_of_table, tables, cross_input, cotangent, up_weight, down_weight
):
    groups, owners = lax.axis_size("grp"), lax.axis_size("tbl")
    batch, depth = cross_input.shape
    rank = down_weight.shape[1]
    slots, rows, _ = tables.shape
    maxlen = next_ids.shape[1] // (slots * owners)
    fits = owners == 4 and groups % 2 == 0 and depth % (16 * groups) == 0 and batch % 16 == 0
    if not fits or rank * 2 != owners * LANES or slots * maxlen % 8 or slots * maxlen > LANES or batch != LANES:
        return plain(
            next_ids,
            next_lengths,
            slot_of_table,
            tables,
            cross_input,
            cotangent,
            up_weight,
            down_weight,
        )
    factor = 1.0 / math.sqrt(batch * groups * owners)
    next_embedded, grad_up, grad_down = fused_step(
        next_ids,
        next_lengths,
        slot_of_table,
        tables,
        cross_input,
        cotangent,
        up_weight,
        down_weight,
        maxlen,
        factor,
    )
    return next_embedded, grad_up, grad_down.T


def solution(mesh):
    return jax.shard_map(
        on_device,
        mesh=mesh,
        in_specs=(
            P(("grp", "tbl"), None),
            P(("grp", "tbl"), None),
            P(),
            P("tbl", None, None),
            P(("grp", "tbl"), None),
            P(("grp", "tbl"), None),
            P(),
            P(),
        ),
        out_specs=(P(("grp", "tbl"), None), P("tbl", "grp"), P("grp", "tbl")),
        check_vma=False,
    )
```

```python
import functools
import math

import jax
import jax.numpy as jnp
from jax import lax
from jax.experimental import pallas as pl
from jax.experimental.pallas import tpu as pltpu
from jax.sharding import PartitionSpec as P

LANES = 128


def pool_kernel(maxlen, idx_ref, tab_ref, out_ref, stage, wide, acc, sem):
    owners, batch, _ = out_ref.shape
    slots, rows, width = tab_ref.shape
    per_line = LANES // maxlen
    lines = batch // per_line
    chunk = 256

    def fetch(s):
        return pltpu.make_async_copy(tab_ref.at[s], stage.at[s % 2], sem.at[s % 2])

    fetch(0).start()
    wide[pl.ds(rows, 8), :] = jnp.zeros((8, width), jnp.float32)
    for s in range(slots):
        if s + 1 < slots:
            fetch(s + 1).start()
        fetch(s).wait()

        @pl.loop(0, rows // chunk)
        def _(c):
            at = pl.ds(pl.multiple_of(c * chunk, chunk), chunk)
            wide[at, :] = stage[s % 2, at, :].astype(jnp.float32)

        @pl.loop(0, owners * lines)
        def _(g):
            src = g // lines
            line = s * lines + g % lines
            for u in range(per_line):
                got = [
                    wide[pl.ds(idx_ref[src, line, u * maxlen + k], 1), :] for k in range(maxlen)
                ]
                while len(got) > 1:
                    got = [a + b for a, b in zip(got[::2], got[1::2])] + (
                        [got[-1]] if len(got) % 2 else []
                    )
                acc[pl.ds(g * per_line + u, 1), :] = got[0]

        for o in range(owners):
            out_ref[o, :, s * width : (s + 1) * width] = acc[
                o * batch : (o + 1) * batch, :
            ].astype(jnp.bfloat16)


def pool(idx, tables, batch, maxlen):
    slots, rows, width = tables.shape
    owners = idx.shape[0]
    return pl.pallas_call(
        functools.partial(pool_kernel, maxlen),
        out_shape=jax.ShapeDtypeStruct((owners, batch, slots * width), jnp.bfloat16),
        in_specs=[
            pl.BlockSpec(memory_space=pltpu.SMEM),
            pl.BlockSpec(memory_space=pl.ANY),
        ],
        out_specs=pl.BlockSpec(memory_space=pltpu.VMEM),
        scratch_shapes=[
            pltpu.VMEM((2, rows, width), jnp.bfloat16),
            pltpu.VMEM((rows + 8, width), jnp.float32),
            pltpu.VMEM((owners * batch, width), jnp.float32),
            pltpu.SemaphoreType.DMA((2,)),
        ],
        compiler_params=pltpu.CompilerParams(vmem_limit_bytes=60 << 20),
        cost_estimate=pl.CostEstimate(
            flops=100_000_000, bytes_accessed=tables.size * 2, transcendentals=0
        ),
        name="pool",
    )(idx, tables)


def order_kernel(slot_ref, got_ref, out_ref):
    owners, batch, wide = got_ref.shape
    feats = slot_ref.shape[0]
    width = out_ref.shape[1] // feats
    slots = wide // width
    for f in range(feats):
        s = slot_ref[f]
        at = pl.ds(pl.multiple_of(lax.rem(s, slots) * width, width), width)
        out_ref[:, f * width : (f + 1) * width] = got_ref[lax.div(s, slots), :, at]


def order(slot_of_table, got, width):
    return pl.pallas_call(
        order_kernel,
        out_shape=jax.ShapeDtypeStruct(
            (got.shape[1], slot_of_table.shape[0] * width), jnp.bfloat16
        ),
        in_specs=[
            pl.BlockSpec(memory_space=pltpu.SMEM),
            pl.BlockSpec(memory_space=pltpu.VMEM),
        ],
        out_specs=pl.BlockSpec(memory_space=pltpu.VMEM),
        name="order",
    )(slot_of_table, got)


def bag_rows(next_ids, next_lengths, slot_of_table, slots, owners, rows):
    batch = next_ids.shape[0]
    slots_all = slots * owners
    maxlen = next_ids.shape[1] // slots_all
    hit = (slot_of_table[:, None] == lax.broadcasted_iota(jnp.int32, (1, slots_all), 1)).astype(
        jnp.int32
    )
    slot_lengths = jnp.sum(next_lengths[:, :, None] * hit[None, :, :], axis=1)
    keep = lax.broadcasted_iota(jnp.int32, (batch, slots_all, maxlen), 2) < slot_lengths[:, :, None]
    idx = jnp.where(keep, next_ids.reshape(batch, slots_all, maxlen), rows)
    return idx.transpose(1, 0, 2).reshape(owners, slots * batch * maxlen // LANES, LANES)


def plain(
    next_ids, next_lengths, slot_of_table, tables, cross_input, cotangent, up_weight, down_weight
):
    batch = next_ids.shape[0]
    owners = lax.axis_size("tbl")
    slots, rows, width = tables.shape
    maxlen = next_ids.shape[1] // (slots * owners)
    idx = bag_rows(next_ids, next_lengths, slot_of_table, slots, owners, rows)
    low = jnp.dot(cross_input, down_weight, preferred_element_type=jnp.float32).astype(jnp.bfloat16)
    dz = (cotangent.astype(jnp.float32) * cross_input.astype(jnp.float32)).astype(jnp.bfloat16)
    dlow = jnp.dot(dz, up_weight.T, preferred_element_type=jnp.float32).astype(jnp.bfloat16)
    total = batch * lax.axis_size("grp") * owners
    factor = 1.0 / math.sqrt(total)
    part_up = jnp.dot(low.T, dz, preferred_element_type=jnp.float32) * factor
    part_down = jnp.dot(cross_input.T, dlow, preferred_element_type=jnp.float32) * factor
    part_up, part_down = part_up.astype(jnp.bfloat16), part_down.astype(jnp.bfloat16)
    owner_up, owner_down = (
        lax.psum_scatter(part_up, "tbl", scatter_dimension=0, tiled=True).astype(jnp.float32),
        lax.psum_scatter(part_down, "tbl", scatter_dimension=1, tiled=True).astype(jnp.float32),
    )
    got_idx = lax.all_to_all(idx, "tbl", split_axis=0, concat_axis=0, tiled=True)
    pooled = pool(got_idx, tables, batch, maxlen)
    returned = lax.all_to_all(pooled, "tbl", split_axis=0, concat_axis=0, tiled=True)
    next_embedded = order(slot_of_table, returned, width)
    grad_up, grad_down = (
        lax.psum_scatter(owner_up, "grp", scatter_dimension=1, tiled=True),
        lax.psum_scatter(owner_down, "grp", scatter_dimension=0, tiled=True),
    )
    return (next_embedded, grad_up, grad_down)


def step_kernel(
    maxlen,
    factor,
    split,
    checkpoints,
    ids_ref,
    len_ref,
    slot_ref,
    tab_ref,
    x_hbm,
    ct_hbm,
    up_hbm,
    down_hbm,
    emb_ref,
    grad_up_ref,
    grad_down_ref,
    x_ref,
    ct_ref,
    up_ref,
    down_ref,
    idx_ref,
    idx_in,
    turned,
    idx_s,
    part,
    c_in,
    a_in,
    b_in,
    a2_in,
    b2_in,
    z_in,
    stage,
    wide,
    acc,
    pooled,
    got,
    tab_sem,
    smem_sem,
    idx_sem,
    core_sem,
    one_sem,
    two_sem,
    z_sem,
    pool_sem,
    load_sem,
):
    owners, zs, _, high, lanes = part.shape
    slots, rows, width = tab_ref.shape
    batch = x_ref.shape[0]
    rank = down_ref.shape[1]
    cols = rank // owners
    group = 32
    chunk = 1024 if rows % 1024 == 0 else 256
    g, t = lax.axis_index("grp"), lax.axis_index("tbl")
    z, x = g // 2, g % 2
    core = t + 1 - 2 * (t % 2)
    far = (t + 2) % owners
    other = 1 - x
    side = g + 1 - 2 * x

    def fetch(s):
        return pltpu.make_async_copy(tab_ref.at[s], stage.at[s % 2], tab_sem.at[s % 2])

    def send(src, dst, sems, n, device):
        return pltpu.make_async_remote_copy(
            src_ref=src,
            dst_ref=dst,
            send_sem=sems.at[0, n],
            recv_sem=sems.at[1, n],
            device_id=device,
            device_id_type=pl.DeviceIdType.MESH,
        )

    loads = [
        pltpu.make_async_copy(a, b, load_sem.at[n])
        for n, (a, b) in enumerate(
            ((x_hbm, x_ref), (down_hbm, down_ref), (ct_hbm, ct_ref), (up_hbm, up_ref))
        )
    ]
    for copy in loads:
        copy.start()
    fetch(0).start()
    barrier = pltpu.get_barrier_semaphore()
    near = [(g, (t + d) % owners) for d in range(1, owners)] + [(side, t)]
    near += [((z + d) % zs * 2 + x, t) for d in range(1, zs)]
    for device in near:
        pl.semaphore_signal(
            barrier, inc=1, device_id=device, device_id_type=pl.DeviceIdType.MESH
        )

    feats, span = slot_ref.shape[0], ids_ref.shape[0]
    each = slots * maxlen
    feat = lax.broadcasted_iota(jnp.int32, (span, feats), 1)
    entry = lax.broadcasted_iota(jnp.int32, (span, feats), 0)
    held_by = jnp.zeros((span, feats), jnp.int32)
    for f in range(feats):
        held_by = jnp.where(feat == f, slot_ref[f], held_by)
    hit = jnp.where(held_by == entry // maxlen, 1.0, 0.0).astype(jnp.bfloat16)
    lens = jnp.dot(
        hit, len_ref[...].astype(jnp.float32).astype(jnp.bfloat16), preferred_element_type=jnp.float32
    )
    place = (lax.broadcasted_iota(jnp.int32, (span, batch), 0) % maxlen).astype(jnp.float32)
    idx = jnp.where(place < lens, ids_ref[...], rows)
    for o in range(owners):
        idx_ref[o] = idx[o * each : (o + 1) * each]

    pl.semaphore_wait(barrier, len(near))

    ids_out = [
        send(idx_ref.at[(t + d) % owners], idx_in.at[t], idx_sem, d - 1, (g, (t + d) % owners))
        for d in range(1, owners)
    ]
    for copy in ids_out:
        copy.start()

    loads[0].wait()
    loads[1].wait()
    low = jnp.dot(x_ref[...], down_ref[...], preferred_element_type=jnp.float32).astype(jnp.bfloat16)
    loads[2].wait()
    dz = (ct_ref[...].astype(jnp.float32) * x_ref[...].astype(jnp.float32)).astype(jnp.bfloat16)
    loads[3].wait()
    dlow = lax.dot_general(
        dz, up_ref[...], (((1,), (1,)), ((), ())), preferred_element_type=jnp.float32
    ).astype(jnp.bfloat16)
    first = (((0,), (0,)), ((), ()))
    for block in range(2 * zs):
        begin = block * high
        edge = begin // LANES * LANES
        stop = -(-(begin + high) // LANES) * LANES
        up = lax.dot_general(dz[:, edge:stop], low, first, preferred_element_type=jnp.float32)
        down = lax.dot_general(
            x_ref[:, edge:stop], dlow, first, preferred_element_type=jnp.float32
        )
        up = (up[begin - edge : begin - edge + high] * factor).astype(jnp.bfloat16)
        down = (down[begin - edge : begin - edge + high] * factor).astype(jnp.bfloat16)
        for o in range(owners):
            part[o, block // 2, block % 2] = jnp.concatenate(
                [up[:, o * cols : (o + 1) * cols], down[:, o * cols : (o + 1) * cols]], axis=1
            )

    cross = [
        send(part.at[core], c_in.at[0], core_sem, 0, (g, core)),
        send(part.at[(core + 2) % owners], c_in.at[1], core_sem, 1, (g, core)),
    ]
    for copy in cross:
        copy.start()

    for copy in ids_out:
        copy.wait()
    idx_in[t] = idx_ref[t]
    for o in range(owners):
        turned[o] = jnp.zeros((batch, LANES), jnp.int32)
        turned[o, :, :each] = idx_in[o].T
    got_ids = [
        pltpu.make_async_copy(
            turned.at[o], idx_s.at[pl.ds(o * batch, batch)], smem_sem.at[o]
        )
        for o in range(owners)
    ]
    for copy in got_ids:
        copy.start()
    for copy in got_ids:
        copy.wait()

    low_rows, high_rows = pl.ds(0, split), pl.ds(split, high - split)

    def add(where, value):
        part[where] = (part[where].astype(jnp.float32) + value.astype(jnp.float32)).astype(
            jnp.bfloat16
        )

    one = [
        send(part.at[far, :, :, low_rows], a_in, one_sem, 0, (g, far)),
        send(part.at[t, :, other, high_rows], b_in.at[0], one_sem, 1, (side, t)),
        send(part.at[far, :, other, high_rows], b_in.at[1], one_sem, 2, (side, t)),
    ]
    two = [
        send(part.at[t, :, other, low_rows], a2_in, two_sem, 0, (side, t)),
        send(part.at[far, :, x, high_rows], b2_in, two_sem, 1, (g, far)),
    ]
    last = [
        send(
            part.at[t, (z + d) % zs, x], z_in.at[d - 1], z_sem, d - 1, ((z + d) % zs * 2 + x, t)
        )
        for d in range(1, zs)
    ]

    def after_core():
        for copy in cross:
            copy.wait()
        for n, o in ((1, far), (0, t)):
            for k in range(zs):
                for j in range(2):
                    add((o, k, j), c_in[n, k, j])
        for copy in one:
            copy.start()

    def after_one():
        for copy in one:
            copy.wait()
        for k in range(zs):
            add((t, k, other, low_rows), a_in[k, other])
            add((far, k, x, high_rows), b_in[1, k])
        for copy in two:
            copy.start()
        for k in range(zs):
            add((t, k, x, low_rows), a_in[k, x])
            add((t, k, x, high_rows), b_in[0, k])

    def after_two():
        for copy in two:
            copy.wait()
        for k in range(zs):
            add((t, k, x, low_rows), a2_in[k])
            add((t, k, x, high_rows), b2_in[k])
        for copy in last:
            copy.start()

    stages = [after_core, after_one, after_two]
    returns = []
    wide[pl.ds(rows, 8), :] = jnp.zeros((8, width), jnp.float32)
    for s in range(slots):
        if s + 1 < slots:
            fetch(s + 1).start()
        fetch(s).wait()

        @pl.loop(0, rows // chunk)
        def _(c):
            at = pl.ds(pl.multiple_of(c * chunk, chunk), chunk)
            wide[at, :] = stage[s % 2, at, :].astype(jnp.float32)

        @pl.loop(0, owners * batch // group)
        def _(i):
            for u in range(group):
                held = [
                    wide[pl.ds(idx_s[i * group + u, s * maxlen + k], 1), :] for k in range(maxlen)
                ]
                while len(held) > 1:
                    held = [a + b for a, b in zip(held[::2], held[1::2])] + (
                        [held[-1]] if len(held) % 2 else []
                    )
                acc[pl.ds(i * group + u, 1), :] = held[0]

        for n, at in enumerate(checkpoints):
            if at == s:
                stages[n]()
        got[t, s] = acc[pl.ds(pl.multiple_of(t * batch, batch), batch), :].astype(jnp.bfloat16)
        for d in range(1, owners):
            o = (t + d) % owners
            pooled[d - 1, s] = acc[pl.ds(pl.multiple_of(o * batch, batch), batch), :].astype(
                jnp.bfloat16
            )
            copy = send(
                pooled.at[d - 1, s], got.at[t, s], pool_sem, s * (owners - 1) + d - 1, (g, o)
            )
            copy.start()
            returns.append(copy)

    for copy in last:
        copy.wait()
    total = part[t, z, x].astype(jnp.float32)
    for d in range(1, zs):
        total += z_in[d - 1].astype(jnp.float32)
    total = total.T
    grad_up_ref[...] = total[:cols]
    grad_down_ref[...] = total[cols:]
    for copy in returns:
        copy.wait()
    for f in range(slot_ref.shape[0]):
        s = slot_ref[f]
        emb_ref[:, f * width : (f + 1) * width] = got[lax.div(s, slots), lax.rem(s, slots)]


def fused_step(
    next_ids, next_lengths, slot_of_table, tables, cross_input, cotangent, up_weight, down_weight, maxlen, factor
):
    groups, owners = lax.axis_size("grp"), lax.axis_size("tbl")
    slots, rows, width = tables.shape
    batch, depth = cross_input.shape
    zs, high = groups // 2, depth // groups
    split = (high // 2 + 15) // 16 * 16
    sems = pltpu.SemaphoreType.DMA
    bf16 = jnp.bfloat16
    any_space = pl.BlockSpec(memory_space=pl.ANY)
    idx_shape = (owners, next_ids.shape[1] // owners, batch)
    half = down_weight.shape[1] // owners
    vmem = pl.BlockSpec(memory_space=pltpu.VMEM)
    checkpoints = (0, min(3, slots - 1), min(5, slots - 1))
    return pl.pallas_call(
        functools.partial(step_kernel, maxlen, factor, split, checkpoints),
        out_shape=(
            jax.ShapeDtypeStruct((batch, slot_of_table.shape[0] * width), bf16),
            jax.ShapeDtypeStruct((half, high), jnp.float32),
            jax.ShapeDtypeStruct((half, high), jnp.float32),
        ),
        in_specs=[
            vmem,
            vmem,
            pl.BlockSpec(memory_space=pltpu.SMEM),
            any_space,
            any_space,
            any_space,
            any_space,
            any_space,
        ],
        out_specs=(vmem, vmem, vmem),
        scratch_shapes=[
            pltpu.VMEM(cross_input.shape, bf16),
            pltpu.VMEM(cotangent.shape, bf16),
            pltpu.VMEM(up_weight.shape, bf16),
            pltpu.VMEM(down_weight.shape, bf16),
            pltpu.VMEM(idx_shape, jnp.int32),
            pltpu.VMEM(idx_shape, jnp.int32),
            pltpu.VMEM((owners, batch, LANES), jnp.int32),
            pltpu.SMEM((owners * batch, LANES), jnp.int32),
            pltpu.VMEM((owners, zs, 2, high, LANES), bf16),
            pltpu.VMEM((2, zs, 2, high, LANES), bf16),
            pltpu.VMEM((zs, 2, split, LANES), bf16),
            pltpu.VMEM((2, zs, high - split, LANES), bf16),
            pltpu.VMEM((zs, split, LANES), bf16),
            pltpu.VMEM((zs, high - split, LANES), bf16),
            pltpu.VMEM((max(zs - 1, 1), high, LANES), bf16),
            pltpu.VMEM((2, rows, width), bf16),
            pltpu.VMEM((rows + 8, width), jnp.float32),
            pltpu.VMEM((owners * batch, width), jnp.float32),
            pltpu.VMEM((owners - 1, slots, batch, width), bf16),
            pltpu.VMEM((owners, slots, batch, width), bf16),
            sems((2,)),
            sems((owners,)),
            sems((2, owners - 1)),
            sems((2, 2)),
            sems((2, 3)),
            sems((2, 2)),
            sems((2, max(zs - 1, 1))),
            sems((2, slots * (owners - 1))),
            sems((4,)),
        ],
        compiler_params=pltpu.CompilerParams(
            collective_id=0, has_side_effects=True, vmem_limit_bytes=56 << 20
        ),
        name="fused_step",
    )(
        next_ids.T,
        next_lengths.T,
        slot_of_table,
        tables,
        cross_input,
        cotangent,
        up_weight,
        down_weight,
    )


def on_device(
    next_ids, next_lengths, slot_of_table, tables, cross_input, cotangent, up_weight, down_weight
):
    groups, owners = lax.axis_size("grp"), lax.axis_size("tbl")
    batch, depth = cross_input.shape
    rank = down_weight.shape[1]
    slots, rows, _ = tables.shape
    maxlen = next_ids.shape[1] // (slots * owners)
    fits = owners == 4 and groups % 2 == 0 and depth % (16 * groups) == 0 and batch % 16 == 0
    if not fits or rank * 2 != owners * LANES or slots * maxlen % 8 or slots * maxlen > LANES or batch != LANES:
        return plain(
            next_ids,
            next_lengths,
            slot_of_table,
            tables,
            cross_input,
            cotangent,
            up_weight,
            down_weight,
        )
    factor = 1.0 / math.sqrt(batch * groups * owners)
    next_embedded, grad_up, grad_down = fused_step(
        next_ids,
        next_lengths,
        slot_of_table,
        tables,
        cross_input,
        cotangent,
        up_weight,
        down_weight,
        maxlen,
        factor,
    )
    return next_embedded, grad_up, grad_down.T


def solution(mesh):
    return jax.shard_map(
        on_device,
        mesh=mesh,
        in_specs=(
            P(("grp", "tbl"), None),
            P(("grp", "tbl"), None),
            P(),
            P("tbl", None, None),
            P(("grp", "tbl"), None),
            P(("grp", "tbl"), None),
            P(),
            P(),
        ),
        out_specs=(P(("grp", "tbl"), None), P("tbl", "grp"), P("grp", "tbl")),
        check_vma=False,
    )
```
